32 devices in a mesh: amp: 32 (over z, y, x, core).
Axes of the slice: x: 2, y: 2, z: 4, core: 2. Of those that a mesh axis runs over, the one named last changes fastest.
Arguments:
- ket_state: float32 [2, 1048576], P(None, 'amp'), may hold values from -6 to 6
- observable: float32 [1048576], P('amp'), may hold values from -6 to 6
- angles: float32 [2, 3], replicated, may hold values from -3.140625 to 3.140625
- gate_kinds: int32 [2, 32], replicated, may hold values from 0 to 2
Outputs:
- bra_state: float32 [2, 1048576], P(None, 'amp')
- grads: float32 [2, 3], replicated
The draws below stay inside these ranges and needn't reach their ends.
Inputs may be any that keep to these rules, and one draw needn't show every extreme that they name: `gate_kinds`: 0 and 1 name rotations about Y with angles[l, 0] and angles[l, 1], 2 a rotation about Z with angles[l, 2]; entries for qubits at or above the number of qubits are not used.
All inputs are finite; a program needn't handle non-finite values.
Results may differ from the reference program's by a relative error of at most 0.0003.
Values sent between devices are 32-bit elements; how exact they have to be, the bound alone decides.
No kernel may reach another device: no remote copies, remote signals or barrier semaphores. Data moves between devices by JAX's collectives and lax.ppermute only.
A program may use at most 128 MiB of HBM per device.

```python
import math
import jax
import jax.numpy as jnp
from jax import lax

AMPS_DEV = 32768
LAYERS = 2
KINDS = 3
QSLOTS = 32
AMPS = 1048576
N_AMP = 32


def set_ends(drawn, own_key, smallest, largest):
    shape = drawn.shape
    place = [jax.random.randint(jax.random.fold_in(own_key, axis), (), 0, shape[axis]) for axis in range(len(shape))]
    drawn = drawn.at[tuple(place)].set(smallest)
    longest = shape.index(max(shape))
    place[longest] = (place[longest] + 1) % shape[longest]
    return drawn.at[tuple(place)].set(largest)


def block_levels(rng, dims, pieces, low, largest):
    def one(position, blocks):
        draws = jax.random.uniform(jax.random.fold_in(jax.random.fold_in(rng, 6), position), (blocks,), jnp.float32, low / len(pieces), largest / len(pieces))
        return jnp.repeat(jnp.exp(draws), dims[position] // blocks).reshape((-1,) + (1,) * (len(dims) - position - 1))

    factor_of = one(*pieces[0])
    for cut in pieces[1:]:
        factor_of = factor_of * one(*cut)
    return factor_of


def normal_values(stream_key, dims, spread, limit, cuts=(), kind=jnp.bfloat16):
    drawn = spread * jax.random.normal(stream_key, dims, jnp.float32)
    if cuts:
        drawn = drawn * block_levels(stream_key, dims, cuts, -0.22, 0.18)
    return jnp.clip(drawn, -limit, limit).astype(kind)


def setup_inputs(seed: int = 0) -> dict:
    streams_of = jax.random.split(jax.random.key(seed), 5)
    return {
        "ket_state": normal_values(streams_of[0], (2, AMPS), 1.0, 6.0, ((1, 32),), jnp.float32),
        "observable": normal_values(streams_of[1], (AMPS,), 1.0, 6.0, ((0, 32),), jnp.float32),
        "angles": jnp.clip(jax.random.uniform(streams_of[2], (LAYERS, KINDS), jnp.float32, -3.140625, 3.140625), -3.140625, 3.140625),
        "gate_kinds": set_ends(jax.random.randint(streams_of[3], (LAYERS, QSLOTS), 0, 3), jax.random.fold_in(streams_of[3], 1), 0, 2).astype(jnp.int32),
    }


def rotate_phase(values, cosine, sine_value):
    return jnp.stack([cosine * values[0] - sine_value * values[1], cosine * values[1] + sine_value * values[0]])

def undo_qubit(ket_state, bra_state, qubit_id, rotation, is_z):
    amp_total = ket_state.shape[1]
    fold_shape = (2, amp_total >> qubit_id + 1, 2, 1 << qubit_id)
    cosine = jnp.cos(0.5 * rotation)
    sine_value = jnp.sin(0.5 * rotation)

    def turn_y(operands):
        folded_ket, folded_bra = operands
        ket_low, ket_high = (folded_ket[:, :, 0], folded_ket[:, :, 1])
        bra_low, bra_high = (folded_bra[:, :, 0], folded_bra[:, :, 1])
        partial_value = 0.5 * jnp.sum(bra_high * ket_low - bra_low * ket_high)
        new_ket = jnp.stack([cosine * ket_low + sine_value * ket_high, cosine * ket_high - sine_value * ket_low], axis=2)
        new_bra = jnp.stack([cosine * bra_low + sine_value * bra_high, cosine * bra_high - sine_value * bra_low], axis=2)
        return (new_ket, new_bra, partial_value)

    def turn_z(operands):
        folded_ket, folded_bra = operands
        ket_low, ket_high = (folded_ket[:, :, 0], folded_ket[:, :, 1])
        bra_low, bra_high = (folded_bra[:, :, 0], folded_bra[:, :, 1])
        partial_value = 0.5 * (jnp.sum(bra_low[0] * ket_low[1] - bra_low[1] * ket_low[0]) - jnp.sum(bra_high[0] * ket_high[1] - bra_high[1] * ket_high[0]))
        new_ket = jnp.stack([rotate_phase(ket_low, cosine, sine_value), rotate_phase(ket_high, cosine, -sine_value)], axis=2)
        new_bra = jnp.stack([rotate_phase(bra_low, cosine, sine_value), rotate_phase(bra_high, cosine, -sine_value)], axis=2)
        return (new_ket, new_bra, partial_value)
    new_ket, new_bra, partial_value = lax.cond(is_z, turn_z, turn_y, (ket_state.reshape(fold_shape), bra_state.reshape(fold_shape)))
    return (new_ket.reshape(2, amp_total), new_bra.reshape(2, amp_total), partial_value)

def reference(ket_state, observable, angles, gate_kinds):
    amp_total = AMPS_DEV * N_AMP
    all_bits = int(amp_total).bit_length() - 1
    bra_state = 2.0 / math.sqrt(amp_total) * observable[None, :] * ket_state
    amp_index = jnp.arange(amp_total, dtype=jnp.int32)
    parity = jnp.zeros((amp_total,), jnp.int32)
    for qubit_id in range(all_bits):
        neighbor = (qubit_id + 1) % all_bits
        parity = parity + (amp_index >> qubit_id & 1) * (amp_index >> neighbor & 1)
    phase_sign = (1 - 2 * (parity & 1)).astype(jnp.float32)
    grads = jnp.zeros((LAYERS, KINDS), jnp.float32)
    kind_range = jnp.arange(KINDS)
    layer_range = jnp.arange(LAYERS)
    for layer_id in reversed(range(LAYERS)):
        ket_state = ket_state * phase_sign[None, :]
        bra_state = bra_state * phase_sign[None, :]
        for qubit_id in range(all_bits):
            kind_id = gate_kinds[layer_id, qubit_id]
            rotation = jnp.sum(jnp.where(kind_range == kind_id, angles[layer_id], 0.0))
            ket_state, bra_state, partial_value = undo_qubit(ket_state, bra_state, qubit_id, rotation, kind_id == 2)
            selector = ((layer_range[:, None] == layer_id) & (kind_range[None, :] == kind_id)).astype(grads.dtype)
            grads = grads + partial_value * selector
    return (bra_state, grads)
```

```python
import functools
import math

import jax
import jax.numpy as jnp
from jax import lax
from jax.experimental import pallas as pl
from jax.experimental.pallas import tpu as pltpu
from jax.sharding import PartitionSpec as P

LANE_BITS = 7
ROW_BITS = 10
TILE = 8


class Frame:
    def __init__(self, local_bits, global_bits):
        self.local_bits = local_bits
        self.global_bits = global_bits
        self.all_bits = local_bits + global_bits
        self.pivot = local_bits - 1 - global_bits
        self.tiles = 1 << (local_bits - ROW_BITS)
        self.rows = self.tiles * TILE
        self.group = 1 << global_bits
        self.chunk = self.rows // self.group
        self.chunked = self.rows % self.group == 0 and self.chunk % TILE == 0

    def first_map(self):
        return {q: ("local", q) if q < self.local_bits else ("device", q - self.local_bits)
                for q in range(self.all_bits)}

    def second_map(self):
        where = {q: ("local", q) for q in range(self.pivot)}
        where[self.local_bits - 1] = ("local", self.pivot)
        for k in range(self.global_bits):
            where[self.local_bits + k] = ("local", self.pivot + 1 + k)
            where[self.pivot if k == self.global_bits - 1 else self.pivot + 1 + k] = ("device", k)
        return where

    def moved_map(self):
        return {pos: self.pivot if pos == self.local_bits - 1 else pos
                for pos in range(self.pivot + 1, self.local_bits)}


def lane_iota():
    return lax.broadcasted_iota(jnp.int32, (TILE, 128), 1)


def sub_iota():
    return lax.broadcasted_iota(jnp.int32, (TILE, 128), 0)


def bit_of(pos):
    if pos < LANE_BITS:
        return lane_iota() >> pos & 1
    return sub_iota() >> (pos - LANE_BITS) & 1


def sign_of(pos):
    return (1 - 2 * bit_of(pos)).astype(jnp.float32)


def shift_up(x, pos):
    if pos < LANE_BITS:
        return pltpu.roll(x, 128 - (1 << pos), 1)
    return pltpu.roll(x, TILE - (1 << (pos - LANE_BITS)), 0)


def shift_down(x, pos):
    if pos < LANE_BITS:
        return pltpu.roll(x, 1 << pos, 1)
    return pltpu.roll(x, 1 << (pos - LANE_BITS), 0)


def flip(x, pos):
    if pos in (LANE_BITS - 1, ROW_BITS - 1):
        return shift_down(x, pos)
    return jnp.where(bit_of(pos) == 0, shift_up(x, pos), shift_down(x, pos))


def entangle(amp, all_bits):
    x = amp & (amp >> 1 | (amp & 1) << (all_bits - 1))
    step = 16
    while step:
        x = x ^ x >> step
        step //= 2
    return (1 - 2 * (x & 1)).astype(jnp.float32)


def position_index(tile):
    return tile << ROW_BITS | sub_iota() << LANE_BITS | lane_iota()


def swap_pivot(tiles, frame):
    half = len(tiles) // 2
    pos = frame.pivot
    out = list(tiles)
    for t in range(half):
        low, high = tiles[t], tiles[t + half]
        if pos >= ROW_BITS:
            bit = 1 << (pos - ROW_BITS)
            if t & bit:
                out[t], out[t - bit + half] = tiles[t - bit + half], tiles[t]
        else:
            keep = bit_of(pos) == 0
            out[t] = jnp.where(keep, low, shift_down(high, pos))
            out[t + half] = jnp.where(keep, shift_up(low, pos), high)
    return out


class Params:
    def __init__(self, table, kinds, layers):
        self.table = table
        self.kinds = kinds
        self.layers = layers

    def gate(self, layer, qubit):
        return (self.table[layer, qubit], self.table[self.layers + layer, qubit],
                self.table[2 * self.layers + layer, qubit])

    def pick(self, layer, qubit, kind):
        return jnp.where(self.kinds[layer, qubit] == kind, 0.5, 0.0)


def turn(re, im, gate, pos, low_tile_bit):
    c, sy, sz = gate
    if pos < ROW_BITS:
        z = sign_of(pos)
        y_part, z_part = sy * z, sz * z
        new_re = [c * a + y_part * flip(a, pos) - z_part * b for a, b in zip(re, im)]
        new_im = [c * b + y_part * flip(b, pos) + z_part * a for a, b in zip(re, im)]
        return new_re, new_im
    bit = 1 << (pos - ROW_BITS - low_tile_bit)
    new_re, new_im = list(re), list(im)
    for t in range(len(re)):
        if t & bit:
            continue
        u = t | bit
        new_re[t] = c * re[t] + sy * re[u] - sz * im[t]
        new_im[t] = c * im[t] + sy * im[u] + sz * re[t]
        new_re[u] = c * re[u] - sy * re[t] + sz * im[u]
        new_im[u] = c * im[u] - sy * im[t] - sz * re[u]
    return new_re, new_im


def sweep(loads, stores, frame, gates):
    tile_bits = frame.tiles.bit_length() - 1
    low = min(3, tile_bits)
    span = 1 << low
    near = [pos for pos in sorted(gates) if LANE_BITS <= pos < ROW_BITS + low]
    far = [pos for pos in sorted(gates) if pos >= ROW_BITS + low]
    load, store = loads, stores
    plans = []
    if near:
        plans.append((near, 0, [[base * span + t for t in range(span)]
                                for base in range(frame.tiles // span)]))
    if far:
        plans.append((far, low, [[base + t * span for t in range(frame.tiles // span)]
                                 for base in range(span)]))
    for positions, low_bit, blocks in plans:
        for block in blocks:
            pairs = [load(t) for t in block]
            re, im = [a for a, _ in pairs], [b for _, b in pairs]
            for pos in positions:
                re, im = turn(re, im, gates[pos], pos, low_bit)
            for t, a, b in zip(block, re, im):
                store(t, a, b)


def split(x):
    high = x.astype(jnp.bfloat16)
    return high, (x - high.astype(jnp.float32)).astype(jnp.bfloat16)


def lane_matrix(params, layer, qubits):
    into = lax.broadcasted_iota(jnp.int32, (128, 128), 0)
    out = lax.broadcasted_iota(jnp.int32, (128, 128), 1)
    real = imag = None
    for pos, qubit in enumerate(qubits):
        c, sy, sz = params.gate(layer, qubit)
        z = (1 - 2 * (out >> pos & 1)).astype(jnp.float32)
        same = (into ^ out) >> pos & 1 == 0
        g_real = jnp.where(same, c, sy * z)
        g_imag = jnp.where(same, sz * z, 0.0)
        if real is None:
            real, imag = g_real, g_imag
        else:
            real, imag = real * g_real - imag * g_imag, real * g_imag + imag * g_real
    top = jnp.concatenate([real, imag], axis=1)
    bottom = jnp.concatenate([-imag, real], axis=1)
    return jnp.concatenate([top, bottom], axis=0)


def lane_turn(x, matrix):
    x_high, x_low = split(x)
    m_high, m_low = split(matrix)
    dot = functools.partial(jnp.dot, preferred_element_type=jnp.float32)
    return dot(x_high, m_high) + (dot(x_low, m_high) + dot(x_high, m_low))


def parts_of(where, qubit, device):
    kind, pos = where[qubit]
    if kind == "device":
        return None, None, (1 - 2 * (device >> pos & 1)).astype(jnp.float32)
    if pos >= ROW_BITS:
        return 1 << (pos - ROW_BITS), None, None
    return None, sign_of(pos), None


def odd(x):
    return bin(x).count("1") & 1


def gather_terms(frame, where, qubits, load_ket, load_bra, params, device):
    n = frame.all_bits
    layers = params.layers
    zero = jnp.zeros((TILE, 128), jnp.float32)
    near, far = [], []
    for q in qubits:
        (far if where[q][1] >= ROW_BITS else near).append(q)
    ratio_mask = {}
    for q in qubits:
        mask = 0
        for other in ((q - 1) % n, (q + 1) % n):
            kind, pos = where[other]
            if kind == "local" and pos >= ROW_BITS:
                mask ^= 1 << (pos - ROW_BITS)
        ratio_mask[q] = mask
    buckets = {q: [None, None] for q in qubits}

    def add(q, side, value):
        old = buckets[q][side]
        buckets[q][side] = value if old is None else old + value

    phases = []
    for t in range(frame.tiles):
        ket_re, ket_im = load_ket(t)
        bra_re, bra_im = load_bra(t)
        phases.append(bra_re * ket_im - bra_im * ket_re)
        for q in near:
            pos = where[q][1]
            value = bra_re * flip(ket_re, pos) + bra_im * flip(ket_im, pos)
            add(q, odd(t & ratio_mask[q]), value)
    for q in far:
        bit = 1 << (where[q][1] - ROW_BITS)
        for t in range(frame.tiles):
            if t & bit:
                continue
            ket_low, ket_high = load_ket(t), load_ket(t | bit)
            bra_low, bra_high = load_bra(t), load_bra(t | bit)
            value = (bra_high[0] * ket_low[0] + bra_high[1] * ket_low[1]) - (
                bra_low[0] * ket_high[0] + bra_low[1] * ket_high[1])
            add(q, odd(t & ratio_mask[q]), value)
    signed = {}
    level = phases
    bit = frame.tiles // 2
    while bit:
        diffs = [level[t] - level[t + bit] for t in range(bit)]
        while len(diffs) > 1:
            half = len(diffs) // 2
            diffs = [diffs[t] + diffs[t + half] for t in range(half)]
        signed[bit] = diffs[0]
        level = [level[t] + level[t + bit] for t in range(bit)]
        bit //= 2
    total = level[0]
    sums = [[zero, zero, zero] for _ in range(layers)]
    for q in qubits:
        pos = where[q][1]
        plus, minus = [zero if b is None else b for b in buckets[q]]
        if pos < ROW_BITS:
            z = sign_of(pos)
            phase = total * z
            last = (plus + minus) * -z
            first = (plus - minus) * -z
        else:
            phase = signed[1 << (pos - ROW_BITS)]
            last = plus + minus
            first = plus - minus
        for other in ((q - 1) % n, (q + 1) % n):
            _, vector, scalar = parts_of(where, other, device)
            if vector is not None:
                first = first * vector
            if scalar is not None:
                first = first * scalar
        for layer in range(layers):
            y_term = last if layer == layers - 1 else first
            for kind in range(2):
                sums[layer][kind] = sums[layer][kind] + params.pick(layer, q, kind) * y_term
            sums[layer][2] = sums[layer][2] + params.pick(layer, q, 2) * phase
    return sums


def rows_of(sums):
    flat = [jnp.sum(tile, axis=0, keepdims=True) for layer in sums for tile in layer]
    flat += [jnp.zeros((1, 128), jnp.float32)] * (TILE - len(flat))
    return jnp.concatenate(flat, axis=0)


def tile_ref(frame, ref, comp, comps):
    def at(t):
        if frame.chunked:
            per = frame.chunk // TILE
            start = comp * frame.chunk + t % per * TILE
            return (t // per, pl.ds(start, TILE), slice(None))
        return (comp, pl.ds(t * TILE, TILE), slice(None))
    return at


def scratch_io(ref, frame, state):
    base = state * frame.rows

    def load(t):
        rows = pl.ds(base + t * TILE, TILE)
        return ref[rows, 0:128], ref[rows, 128:256]

    def store(t, re, im):
        rows = pl.ds(base + t * TILE, TILE)
        ref[rows, 0:128] = re
        ref[rows, 128:256] = im

    return load, store


def first_kernel(frame, layers, dev_ref, table, kinds, ket_ref, obs_ref, out_ref, sums_ref, work):
    device = dev_ref[0]
    params = Params(table, kinds, layers)
    layer = layers - 1
    scale = 2.0 / math.sqrt(1 << frame.all_bits)
    load_ket, store_ket = scratch_io(work, frame, 0)
    load_bra, store_bra = scratch_io(work, frame, 1)
    for t in range(frame.tiles):
        sign = entangle(device << frame.local_bits | position_index(t), frame.all_bits)
        re = ket_ref[pl.ds(2 * TILE * t, TILE, stride=2), :] * sign
        im = ket_ref[pl.ds(2 * TILE * t + 1, TILE, stride=2), :] * sign
        store_ket(t, re, im)
        factor = obs_ref[pl.ds(TILE * t, TILE), :] * scale
        store_bra(t, re * factor, im * factor)
    work[...] = lane_turn(work[...], lane_matrix(params, layer, range(LANE_BITS)))
    gates = {pos: params.gate(layer, pos) for pos in range(LANE_BITS, frame.local_bits)}
    sweep(load_ket, store_ket, frame, gates)
    sweep(load_bra, store_bra, frame, gates)
    moved = list(range(frame.pivot, frame.local_bits - 1))
    sums = gather_terms(frame, frame.first_map(), moved, load_ket, load_bra, params, device)
    sums_ref[...] = rows_of(sums)
    for state, load in enumerate((load_ket, load_bra)):
        pairs = [load(t) for t in range(frame.tiles)]
        for part in range(2):
            tiles = swap_pivot([pair[part] for pair in pairs], frame)
            at = tile_ref(frame, out_ref, 2 * state + part, 4)
            for t in range(frame.tiles):
                out_ref[at(t)] = tiles[t]


def middle_kernel(frame, layers, dev_ref, table, kinds, in_ref, sums_ref, out_ref, work, *flat_out):
    device = dev_ref[0]
    params = Params(table, kinds, layers)
    load_ket, store_ket = scratch_io(work, frame, 0)
    load_bra, store_bra = scratch_io(work, frame, 1)
    where = frame.second_map()
    placed = {pos: q for q, (kind, pos) in where.items() if kind == "local"}
    at = [tile_ref(frame, in_ref, comp, 4) for comp in range(4)]
    for t in range(frame.tiles):
        store_ket(t, in_ref[at[0](t)], in_ref[at[1](t)])
        store_bra(t, in_ref[at[2](t)], in_ref[at[3](t)])
    lane_gates = [pos for pos in range(frame.pivot + 1, frame.local_bits) if pos < LANE_BITS]
    assert not lane_gates
    gates = {pos: params.gate(layers - 1, placed[pos])
             for pos in range(frame.pivot + 1, frame.local_bits)}
    sweep(load_ket, store_ket, frame, gates)
    sweep(load_bra, store_bra, frame, gates)
    qubits = [placed[pos] for pos in range(frame.local_bits)]
    sums = gather_terms(frame, where, qubits, load_ket, load_bra, params, device)
    partial = sums_ref[...] + rows_of(sums)
    g = frame.global_bits
    high = device >> (g - 1) & 1
    base = (device & (1 << (g - 1)) - 1) << (frame.pivot + 1) | high << frame.pivot
    for t in range(frame.tiles):
        pos = position_index(t)
        amp = (base | pos & (1 << frame.pivot) - 1
               | (pos >> frame.pivot & 1) << (frame.local_bits - 1)
               | pos >> (frame.pivot + 1) << frame.local_bits)
        sign = entangle(amp, frame.all_bits)
        re, im = load_bra(t)
        store_bra(t, re * sign, im * sign)
    bra_rows = pl.ds(frame.rows, frame.rows)
    lane_qubits = [placed[pos] for pos in range(LANE_BITS)]
    lane_on = [placed[pos] for pos in range(LANE_BITS)]
    work[bra_rows, :] = lane_turn(work[bra_rows, :], lane_matrix(params, 0, lane_on))
    gates = {pos: params.gate(0, placed[pos]) for pos in range(LANE_BITS, frame.local_bits)}
    sweep(load_bra, store_bra, frame, gates)
    at = [tile_ref(frame, out_ref, comp, 2) for comp in range(2)]
    for t in range(frame.tiles):
        re, im = load_bra(t)
        out_ref[at[0](t)] = re
        out_ref[at[1](t)] = im
    if frame.chunked:
        for j in range(frame.group):
            out_ref[j, pl.ds(2 * frame.chunk, TILE), :] = partial
    else:
        flat_out[0][...] = partial


def last_kernel(frame, layers, table, kinds, in_ref, sums_ref, bra_ref, grads_ref, work):
    params = Params(table, kinds, layers)
    load, store = scratch_io(work, frame, 0)
    at = [tile_ref(frame, in_ref, comp, 2) for comp in range(2)]
    for t in range(frame.tiles):
        store(t, in_ref[at[0](t)], in_ref[at[1](t)])
    gates = {pos: params.gate(0, q) for pos, q in frame.moved_map().items()}
    sweep(load, store, frame, gates)
    pairs = [load(t) for t in range(frame.tiles)]
    for part in range(2):
        tiles = swap_pivot([pair[part] for pair in pairs], frame)
        for t in range(frame.tiles):
            bra_ref[pl.ds(2 * TILE * t + part, TILE, stride=2), :] = tiles[t]
    total = None
    for j in range(frame.group):
        part = in_ref[j, pl.ds(2 * frame.chunk, TILE), :] if frame.chunked else sums_ref[j]
        total = part if total is None else total + part
    for layer in range(layers):
        for kind in range(3):
            row = 3 * layer + kind
            grads_ref[layer, kind] = jnp.sum(total[row:row + 1, :])


def on_device(ket_state, observable, angles, gate_kinds):
    amp_count = ket_state.shape[1]
    local_bits = amp_count.bit_length() - 1
    group = lax.axis_size("amp")
    frame = Frame(local_bits, group.bit_length() - 1)
    layers = angles.shape[0]
    rows = frame.rows
    device = lax.axis_index("amp").astype(jnp.int32).reshape(1)
    chosen = gate_kinds[:, :, None] == jnp.arange(angles.shape[1])[None, None, :]
    half = 0.5 * jnp.sum(jnp.where(chosen, angles[:, None, :], 0.0), axis=-1)
    cosine, sine = jnp.cos(half), jnp.sin(half)
    is_z = gate_kinds == 2
    table = jnp.concatenate(
        [cosine, jnp.where(is_z, 0.0, sine), jnp.where(is_z, sine, 0.0)], axis=0)
    smem = pl.BlockSpec(memory_space=pltpu.SMEM)
    vmem = pl.BlockSpec(memory_space=pltpu.VMEM)
    f32 = jnp.float32

    def packed(comps, extra):
        if frame.chunked:
            return jax.ShapeDtypeStruct((group, comps * frame.chunk + extra, 128), f32)
        return jax.ShapeDtypeStruct((comps, rows, 128), f32)

    def exchange(x):
        return lax.all_to_all(x, "amp", 0, 0, tiled=True)

    def to_chunks(x):
        comps = x.shape[0]
        return x.reshape(comps, group, rows * 128 // group).transpose(1, 0, 2)

    def from_chunks(x):
        return x.transpose(1, 0, 2).reshape(x.shape[1], rows, 128)

    ket_rows = ket_state.reshape(2, rows, 128).transpose(1, 0, 2).reshape(2 * rows, 128)
    obs_rows = observable.reshape(rows, 128)
    work = pltpu.VMEM((2 * rows, 256), f32)
    tile = jax.ShapeDtypeStruct((TILE, 128), f32)
    sent, sums = pl.pallas_call(
        functools.partial(first_kernel, frame, layers),
        in_specs=[smem, smem, smem, vmem, vmem],
        out_specs=(vmem, vmem),
        out_shape=(packed(4, 0), tile),
        scratch_shapes=[work],
        name="first_kernel",
    )(device, table, gate_kinds, ket_rows, obs_rows)
    if frame.chunked:
        got = exchange(sent)
    else:
        got = from_chunks(exchange(to_chunks(sent)))
    outs = (packed(2, TILE),) if frame.chunked else (packed(2, TILE), tile)
    back = pl.pallas_call(
        functools.partial(
            middle_kernel if frame.chunked else middle_flat, frame, layers),
        in_specs=[smem, smem, smem, vmem, vmem],
        out_specs=(vmem,) * len(outs),
        out_shape=outs,
        scratch_shapes=[work],
        name="middle_kernel",
    )(device, table, gate_kinds, got, sums)
    if frame.chunked:
        final = exchange(back[0])
        parts = jnp.zeros((1, TILE, 128), f32)
    else:
        final = from_chunks(exchange(to_chunks(back[0])))
        parts = lax.all_gather(back[1], "amp")
    bra_rows, grads = pl.pallas_call(
        functools.partial(last_kernel, frame, layers),
        in_specs=[smem, smem, vmem, vmem],
        out_specs=(vmem, smem),
        out_shape=(jax.ShapeDtypeStruct((2 * rows, 128), f32),
                   jax.ShapeDtypeStruct((layers, 3), f32)),
        scratch_shapes=[pltpu.VMEM((rows, 256), f32)],
        name="last_kernel",
    )(table, gate_kinds, final, parts)
    bra = bra_rows.reshape(rows, 2, 128).transpose(1, 0, 2).reshape(2, amp_count)
    return bra, grads


def middle_flat(frame, layers, dev_ref, table, kinds, in_ref, sums_ref, out_ref, part_ref, work):
    middle_kernel(frame, layers, dev_ref, table, kinds, in_ref, sums_ref, out_ref, work, part_ref)


def solution(mesh):
    placed = (P(None, "amp"), P("amp"), P(), P())
    return jax.shard_map(
        on_device, mesh=mesh, in_specs=placed, out_specs=(P(None, "amp"), P()), check_vma=False
    )
```

```python
import functools
import math

import jax
import jax.numpy as jnp
from jax import lax
from jax.experimental import pallas as pl
from jax.experimental.pallas import tpu as pltpu
from jax.sharding import PartitionSpec as P

LANE_BITS = 7
ROW_BITS = 10
TILE = 8


class Frame:
    def __init__(self, local_bits, global_bits):
        self.local_bits = local_bits
        self.global_bits = global_bits
        self.all_bits = local_bits + global_bits
        self.pivot = local_bits - 1 - global_bits
        self.tiles = 1 << (local_bits - ROW_BITS)
        self.rows = self.tiles * TILE
        self.group = 1 << global_bits
        self.chunk = self.rows // self.group
        self.chunked = self.rows % self.group == 0 and self.chunk % TILE == 0

    def first_map(self):
        return {q: ("local", q) if q < self.local_bits else ("device", q - self.local_bits)
                for q in range(self.all_bits)}

    def second_map(self):
        where = {q: ("local", q) for q in range(self.pivot)}
        where[self.local_bits - 1] = ("local", self.pivot)
        for k in range(self.global_bits):
            where[self.local_bits + k] = ("local", self.pivot + 1 + k)
            where[self.pivot if k == self.global_bits - 1 else self.pivot + 1 + k] = ("device", k)
        return where

    def moved_map(self):
        return {pos: self.pivot if pos == self.local_bits - 1 else pos
                for pos in range(self.pivot + 1, self.local_bits)}


def lane_iota():
    return lax.broadcasted_iota(jnp.int32, (TILE, 128), 1)


def sub_iota():
    return lax.broadcasted_iota(jnp.int32, (TILE, 128), 0)


def bit_of(pos):
    if pos < LANE_BITS:
        return lane_iota() >> pos & 1
    return sub_iota() >> (pos - LANE_BITS) & 1


def sign_of(pos):
    return (1 - 2 * bit_of(pos)).astype(jnp.float32)


def shift_up(x, pos):
    if pos < LANE_BITS:
        return pltpu.roll(x, 128 - (1 << pos), 1)
    return pltpu.roll(x, TILE - (1 << (pos - LANE_BITS)), 0)


def shift_down(x, pos):
    if pos < LANE_BITS:
        return pltpu.roll(x, 1 << pos, 1)
    return pltpu.roll(x, 1 << (pos - LANE_BITS), 0)


def flip(x, pos):
    if pos in (LANE_BITS - 1, ROW_BITS - 1):
        return shift_down(x, pos)
    return jnp.where(bit_of(pos) == 0, shift_up(x, pos), shift_down(x, pos))


def entangle(amp, all_bits):
    x = amp & (amp >> 1 | (amp & 1) << (all_bits - 1))
    step = 16
    while step:
        x = x ^ x >> step
        step //= 2
    return (1 - 2 * (x & 1)).astype(jnp.float32)


def position_index(tile):
    return tile << ROW_BITS | sub_iota() << LANE_BITS | lane_iota()


def swap_pivot(tiles, frame):
    half = len(tiles) // 2
    pos = frame.pivot
    out = list(tiles)
    for t in range(half):
        low, high = tiles[t], tiles[t + half]
        if pos >= ROW_BITS:
            bit = 1 << (pos - ROW_BITS)
            if t & bit:
                out[t], out[t - bit + half] = tiles[t - bit + half], tiles[t]
        else:
            keep = bit_of(pos) == 0
            out[t] = jnp.where(keep, low, shift_down(high, pos))
            out[t + half] = jnp.where(keep, shift_up(low, pos), high)
    return out


def polynomial(x, coefficients):
    total = jnp.full_like(x, coefficients[-1])
    for value in coefficients[-2::-1]:
        total = total * x + value
    return total


def half_turn(angle):
    x = jnp.full((TILE, 128), 0.5, jnp.float32) * angle
    square = x * x
    cosine = polynomial(square, [(-1) ** k / math.factorial(2 * k) for k in range(9)])
    sine = x * polynomial(square, [(-1) ** k / math.factorial(2 * k + 1) for k in range(8)])
    return cosine, sine


class Params:
    def __init__(self, angles, kinds, layers):
        self.kinds = kinds
        self.layers = layers
        self.turns = {}
        self.angles = angles

    def turn(self, layer, kind):
        if (layer, kind) not in self.turns:
            self.turns[layer, kind] = half_turn(self.angles[layer, kind])
        return self.turns[layer, kind]

    def gate(self, layer, qubit):
        kind = self.kinds[layer, qubit]
        (c0, s0), (c1, s1), (c2, s2) = [self.turn(layer, k) for k in range(3)]
        is_z = kind == 2
        c = jnp.where(is_z, c2, jnp.where(kind == 1, c1, c0))
        sy = jnp.where(is_z, 0.0, jnp.where(kind == 1, s1, s0))
        return c, sy, jnp.where(is_z, s2, 0.0)

    def pick(self, layer, qubit, kind):
        return jnp.where(self.kinds[layer, qubit] == kind, 0.5, 0.0)


def turn(re, im, gate, pos, low_tile_bit):
    c, sy, sz = gate
    if pos < ROW_BITS:
        z = sign_of(pos)
        y_part, z_part = sy * z, sz * z
        new_re = [c * a + y_part * flip(a, pos) - z_part * b for a, b in zip(re, im)]
        new_im = [c * b + y_part * flip(b, pos) + z_part * a for a, b in zip(re, im)]
        return new_re, new_im
    bit = 1 << (pos - ROW_BITS - low_tile_bit)
    new_re, new_im = list(re), list(im)
    for t in range(len(re)):
        if t & bit:
            continue
        u = t | bit
        new_re[t] = c * re[t] + sy * re[u] - sz * im[t]
        new_im[t] = c * im[t] + sy * im[u] + sz * re[t]
        new_re[u] = c * re[u] - sy * re[t] + sz * im[u]
        new_im[u] = c * im[u] - sy * im[t] - sz * re[u]
    return new_re, new_im


def sweep(loads, stores, frame, gates):
    tile_bits = frame.tiles.bit_length() - 1
    low = min(3, tile_bits)
    span = 1 << low
    near = [pos for pos in sorted(gates) if LANE_BITS <= pos < ROW_BITS + low]
    far = [pos for pos in sorted(gates) if pos >= ROW_BITS + low]
    load, store = loads, stores
    plans = []
    if near:
        plans.append((near, 0, [[base * span + t for t in range(span)]
                                for base in range(frame.tiles // span)]))
    if far:
        plans.append((far, low, [[base + t * span for t in range(frame.tiles // span)]
                                 for base in range(span)]))
    for positions, low_bit, blocks in plans:
        for block in blocks:
            pairs = [load(t) for t in block]
            re, im = [a for a, _ in pairs], [b for _, b in pairs]
            for pos in positions:
                re, im = turn(re, im, gates[pos], pos, low_bit)
            for t, a, b in zip(block, re, im):
                store(t, a, b)


def split(x):
    high = x.astype(jnp.bfloat16)
    return high, (x - high.astype(jnp.float32)).astype(jnp.bfloat16)


def lane_matrix(params, layer, qubits):
    into = lax.broadcasted_iota(jnp.int32, (128, 128), 0)
    out = lax.broadcasted_iota(jnp.int32, (128, 128), 1)
    real = imag = None
    for pos, qubit in enumerate(qubits):
        c, sy, sz = [jnp.concatenate([v] * 16, axis=0) for v in params.gate(layer, qubit)]
        z = (1 - 2 * (out >> pos & 1)).astype(jnp.float32)
        same = (into ^ out) >> pos & 1 == 0
        g_real = jnp.where(same, c, sy * z)
        g_imag = jnp.where(same, sz * z, 0.0)
        if real is None:
            real, imag = g_real, g_imag
        else:
            real, imag = real * g_real - imag * g_imag, real * g_imag + imag * g_real
    top = jnp.concatenate([real, imag], axis=1)
    bottom = jnp.concatenate([-imag, real], axis=1)
    return jnp.concatenate([top, bottom], axis=0)


def lane_turn(x, matrix):
    x_high, x_low = split(x)
    m_high, m_low = split(matrix)
    dot = functools.partial(jnp.dot, preferred_element_type=jnp.float32)
    return dot(x_high, m_high) + (dot(x_low, m_high) + dot(x_high, m_low))


def parts_of(where, qubit, device):
    kind, pos = where[qubit]
    if kind == "device":
        return None, None, (1 - 2 * (device >> pos & 1)).astype(jnp.float32)
    if pos >= ROW_BITS:
        return 1 << (pos - ROW_BITS), None, None
    return None, sign_of(pos), None


def odd(x):
    return bin(x).count("1") & 1


def gather_terms(frame, where, qubits, load_ket, load_bra, params, device):
    n = frame.all_bits
    layers = params.layers
    zero = jnp.zeros((TILE, 128), jnp.float32)
    near, far = [], []
    for q in qubits:
        (far if where[q][1] >= ROW_BITS else near).append(q)
    ratio_mask = {}
    for q in qubits:
        mask = 0
        for other in ((q - 1) % n, (q + 1) % n):
            kind, pos = where[other]
            if kind == "local" and pos >= ROW_BITS:
                mask ^= 1 << (pos - ROW_BITS)
        ratio_mask[q] = mask
    buckets = {q: [None, None] for q in qubits}

    def add(q, side, value):
        old = buckets[q][side]
        buckets[q][side] = value if old is None else old + value

    phases = []
    for t in range(frame.tiles):
        ket_re, ket_im = load_ket(t)
        bra_re, bra_im = load_bra(t)
        phases.append(bra_re * ket_im - bra_im * ket_re)
        for q in near:
            pos = where[q][1]
            value = bra_re * flip(ket_re, pos) + bra_im * flip(ket_im, pos)
            add(q, odd(t & ratio_mask[q]), value)
    for q in far:
        bit = 1 << (where[q][1] - ROW_BITS)
        for t in range(frame.tiles):
            if t & bit:
                continue
            ket_low, ket_high = load_ket(t), load_ket(t | bit)
            bra_low, bra_high = load_bra(t), load_bra(t | bit)
            value = (bra_high[0] * ket_low[0] + bra_high[1] * ket_low[1]) - (
                bra_low[0] * ket_high[0] + bra_low[1] * ket_high[1])
            add(q, odd(t & ratio_mask[q]), value)
    signed = {}
    level = phases
    bit = frame.tiles // 2
    while bit:
        diffs = [level[t] - level[t + bit] for t in range(bit)]
        while len(diffs) > 1:
            half = len(diffs) // 2
            diffs = [diffs[t] + diffs[t + half] for t in range(half)]
        signed[bit] = diffs[0]
        level = [level[t] + level[t + bit] for t in range(bit)]
        bit //= 2
    total = level[0]
    sums = [[zero, zero, zero] for _ in range(layers)]
    for q in qubits:
        pos = where[q][1]
        plus, minus = [zero if b is None else b for b in buckets[q]]
        if pos < ROW_BITS:
            z = sign_of(pos)
            phase = total * z
            last = (plus + minus) * -z
            first = (plus - minus) * -z
        else:
            phase = signed[1 << (pos - ROW_BITS)]
            last = plus + minus
            first = plus - minus
        for other in ((q - 1) % n, (q + 1) % n):
            _, vector, scalar = parts_of(where, other, device)
            if vector is not None:
                first = first * vector
            if scalar is not None:
                first = first * scalar
        for layer in range(layers):
            y_term = last if layer == layers - 1 else first
            for kind in range(2):
                sums[layer][kind] = sums[layer][kind] + params.pick(layer, q, kind) * y_term
            sums[layer][2] = sums[layer][2] + params.pick(layer, q, 2) * phase
    return sums


def one_row(tile):
    for step in (64, 32, 16):
        tile = tile + pltpu.roll(tile, step, 1)
    return jnp.sum(jnp.where(lane_iota() >> 4 == sub_iota(), tile, 0.0), axis=0, keepdims=True)


def rows_of(sums):
    flat = [jnp.sum(tile, axis=0, keepdims=True) for layer in sums for tile in layer]
    flat += [jnp.zeros((1, 128), jnp.float32)] * (TILE - len(flat))
    return jnp.concatenate(flat, axis=0)


def back_ref(frame, comp):
    def at(t):
        if frame.chunked:
            per = frame.chunk // TILE
            start = t // per * (2 * frame.chunk + 1) + comp * frame.chunk + t % per * TILE
            return (pl.ds(start, TILE), slice(None))
        return (comp, pl.ds(t * TILE, TILE), slice(None))
    return at


def tile_ref(frame, comp):
    def at(t):
        if frame.chunked:
            per = frame.chunk // TILE
            start = comp * frame.chunk + t % per * TILE
            return (t // per, pl.ds(start, TILE), slice(None))
        return (comp, pl.ds(t * TILE, TILE), slice(None))
    return at


def scratch_io(ref, frame, state):
    base = state * frame.rows

    def load(t):
        rows = pl.ds(base + t * TILE, TILE)
        return ref[rows, 0:128], ref[rows, 128:256]

    def store(t, re, im):
        rows = pl.ds(base + t * TILE, TILE)
        ref[rows, 0:128] = re
        ref[rows, 128:256] = im

    return load, store


def first_kernel(frame, layers, dev_ref, angles, kinds, ket_ref, obs_ref, out_ref, sums_ref, work):
    device = dev_ref[0]
    params = Params(angles, kinds, layers)
    layer = layers - 1
    scale = 2.0 / math.sqrt(1 << frame.all_bits)
    load_ket, store_ket = scratch_io(work, frame, 0)
    load_bra, store_bra = scratch_io(work, frame, 1)
    for t in range(frame.tiles):
        sign = entangle(device << frame.local_bits | position_index(t), frame.all_bits)
        re = ket_ref[pl.ds(2 * TILE * t, TILE, stride=2), :] * sign
        im = ket_ref[pl.ds(2 * TILE * t + 1, TILE, stride=2), :] * sign
        store_ket(t, re, im)
        factor = obs_ref[pl.ds(TILE * t, TILE), :] * scale
        store_bra(t, re * factor, im * factor)
    work[...] = lane_turn(work[...], lane_matrix(params, layer, range(LANE_BITS)))
    gates = {pos: params.gate(layer, pos) for pos in range(LANE_BITS, frame.local_bits)}
    sweep(load_ket, store_ket, frame, gates)
    sweep(load_bra, store_bra, frame, gates)
    moved = list(range(frame.pivot, frame.local_bits - 1))
    sums = gather_terms(frame, frame.first_map(), moved, load_ket, load_bra, params, device)
    sums_ref[...] = rows_of(sums)
    for state, load in enumerate((load_ket, load_bra)):
        pairs = [load(t) for t in range(frame.tiles)]
        for part in range(2):
            tiles = swap_pivot([pair[part] for pair in pairs], frame)
            at = tile_ref(frame, 2 * state + part)
            for t in range(frame.tiles):
                out_ref[at(t)] = tiles[t]


def middle_kernel(frame, layers, dev_ref, angles, kinds, in_ref, sums_ref, out_ref, work, *flat_out):
    device = dev_ref[0]
    params = Params(angles, kinds, layers)
    load_ket, store_ket = scratch_io(work, frame, 0)
    load_bra, store_bra = scratch_io(work, frame, 1)
    where = frame.second_map()
    placed = {pos: q for q, (kind, pos) in where.items() if kind == "local"}
    at = [tile_ref(frame, comp) for comp in range(4)]
    for t in range(frame.tiles):
        store_ket(t, in_ref[at[0](t)], in_ref[at[1](t)])
        store_bra(t, in_ref[at[2](t)], in_ref[at[3](t)])
    assert frame.pivot + 1 >= LANE_BITS
    gates = {pos: params.gate(layers - 1, placed[pos])
             for pos in range(frame.pivot + 1, frame.local_bits)}
    sweep(load_ket, store_ket, frame, gates)
    sweep(load_bra, store_bra, frame, gates)
    qubits = [placed[pos] for pos in range(frame.local_bits)]
    sums = gather_terms(frame, where, qubits, load_ket, load_bra, params, device)
    partial = one_row(sums_ref[...] + rows_of(sums))
    g = frame.global_bits
    high = device >> (g - 1) & 1
    base = (device & (1 << (g - 1)) - 1) << (frame.pivot + 1) | high << frame.pivot
    for t in range(frame.tiles):
        pos = position_index(t)
        amp = (base | pos & (1 << frame.pivot) - 1
               | (pos >> frame.pivot & 1) << (frame.local_bits - 1)
               | pos >> (frame.pivot + 1) << frame.local_bits)
        sign = entangle(amp, frame.all_bits)
        re, im = load_bra(t)
        store_bra(t, re * sign, im * sign)
    bra_rows = pl.ds(frame.rows, frame.rows)
    lane_on = [placed[pos] for pos in range(LANE_BITS)]
    work[bra_rows, :] = lane_turn(work[bra_rows, :], lane_matrix(params, 0, lane_on))
    gates = {pos: params.gate(0, placed[pos]) for pos in range(LANE_BITS, frame.local_bits)}
    sweep(load_bra, store_bra, frame, gates)
    at = [back_ref(frame, comp) for comp in range(2)]
    for t in range(frame.tiles):
        re, im = load_bra(t)
        out_ref[at[0](t)] = re
        out_ref[at[1](t)] = im
    if frame.chunked:
        for j in range(frame.group):
            row = (j + 1) * (2 * frame.chunk + 1) - 1
            out_ref[pl.ds(row, 1), :] = partial
    else:
        flat_out[0][...] = partial


def last_kernel(frame, layers, angles, kinds, in_ref, *refs):
    *sums_ref, bra_ref, grads_ref, work = refs
    params = Params(angles, kinds, layers)
    load, store = scratch_io(work, frame, 0)
    at = [back_ref(frame, comp) for comp in range(2)]
    for t in range(frame.tiles):
        store(t, in_ref[at[0](t)], in_ref[at[1](t)])
    gates = {pos: params.gate(0, q) for pos, q in frame.moved_map().items()}
    sweep(load, store, frame, gates)
    pairs = [load(t) for t in range(frame.tiles)]
    for part in range(2):
        tiles = swap_pivot([pair[part] for pair in pairs], frame)
        for t in range(frame.tiles):
            bra_ref[pl.ds(2 * TILE * t + part, TILE, stride=2), :] = tiles[t]
    if frame.chunked:
        step = 2 * frame.chunk + 1
        rows = in_ref[pl.ds(step - 1, frame.group, stride=step), :]
    else:
        rows = sums_ref[0][:, 0, :]
    total = jnp.sum(rows, axis=0, keepdims=True)
    owner = lax.broadcasted_iota(jnp.int32, (1, 128), 1) >> 4
    for layer in range(layers):
        for kind in range(3):
            own = jnp.where(owner == 3 * layer + kind, total, 0.0)
            grads_ref[layer, kind] = jnp.sum(own)


def on_device(ket_state, observable, angles, gate_kinds):
    amp_count = ket_state.shape[1]
    local_bits = amp_count.bit_length() - 1
    group = lax.axis_size("amp")
    frame = Frame(local_bits, group.bit_length() - 1)
    layers = angles.shape[0]
    rows = frame.rows
    device = lax.axis_index("amp").astype(jnp.int32).reshape(1)
    smem = pl.BlockSpec(memory_space=pltpu.SMEM)
    vmem = pl.BlockSpec(memory_space=pltpu.VMEM)
    f32 = jnp.float32

    def flat(comps):
        return jax.ShapeDtypeStruct((comps, rows, 128), f32)

    def exchange(x):
        return lax.all_to_all(x, "amp", 0, 0, tiled=True)

    def to_chunks(x):
        comps = x.shape[0]
        return x.reshape(comps, group, rows * 128 // group).transpose(1, 0, 2)

    def from_chunks(x):
        return x.transpose(1, 0, 2).reshape(x.shape[1], rows, 128)

    ket_rows = ket_state.reshape(2, rows, 128).transpose(1, 0, 2).reshape(2 * rows, 128)
    obs_rows = observable.reshape(rows, 128)
    work = pltpu.VMEM((2 * rows, 256), f32)
    tile = jax.ShapeDtypeStruct((TILE, 128), f32)
    sent, sums = pl.pallas_call(
        functools.partial(first_kernel, frame, layers),
        in_specs=[smem, smem, smem, vmem, vmem],
        out_specs=(vmem, vmem),
        out_shape=(
            jax.ShapeDtypeStruct((group, 4 * frame.chunk, 128), f32) if frame.chunked else flat(4),
            tile),
        scratch_shapes=[work],
        name="first_kernel",
    )(device, angles, gate_kinds, ket_rows, obs_rows)
    if frame.chunked:
        got = exchange(sent)
    else:
        got = from_chunks(exchange(to_chunks(sent)))
    step = 2 * frame.chunk + 1
    if frame.chunked:
        outs = (jax.ShapeDtypeStruct((group * step, 128), f32),)
    else:
        outs = (flat(2), jax.ShapeDtypeStruct((1, 128), f32))
    back = pl.pallas_call(
        functools.partial(
            middle_kernel if frame.chunked else middle_flat, frame, layers),
        in_specs=[smem, smem, smem, vmem, vmem],
        out_specs=(vmem,) * len(outs),
        out_shape=outs,
        scratch_shapes=[work],
        name="middle_kernel",
    )(device, angles, gate_kinds, got, sums)
    if frame.chunked:
        final = exchange(back[0].reshape(group, step, 1, 128)).reshape(group * step, 128)
        operands = (final,)
    else:
        final = from_chunks(exchange(to_chunks(back[0])))
        operands = (final, lax.all_gather(back[1], "amp"))
    bra_rows, grads = pl.pallas_call(
        functools.partial(last_kernel, frame, layers),
        in_specs=[smem, smem] + [vmem] * len(operands),
        out_specs=(vmem, smem),
        out_shape=(jax.ShapeDtypeStruct((2 * rows, 128), f32),
                   jax.ShapeDtypeStruct((layers, 3), f32)),
        scratch_shapes=[pltpu.VMEM((rows, 256), f32)],
        name="last_kernel",
    )(angles, gate_kinds, *operands)
    bra = bra_rows.reshape(rows, 2, 128).transpose(1, 0, 2).reshape(2, amp_count)
    return bra, grads


def middle_flat(frame, layers, dev_ref, angles, kinds, in_ref, sums_ref, out_ref, part_ref, work):
    middle_kernel(frame, layers, dev_ref, angles, kinds, in_ref, sums_ref, out_ref, work, part_ref)


def solution(mesh):
    placed = (P(None, "amp"), P("amp"), P(), P())
    return jax.shard_map(
        on_device, mesh=mesh, in_specs=placed, out_specs=(P(None, "amp"), P()), check_vma=False
    )
```

```python
import functools
import math

import jax
import jax.numpy as jnp
from jax import lax
from jax.experimental import pallas as pl
from jax.experimental.pallas import tpu as pltpu
from jax.sharding import PartitionSpec as P

LANE_BITS = 7
ROW_BITS = 10
TILE = 8


class Frame:
    def __init__(self, local_bits, global_bits):
        self.local_bits = local_bits
        self.global_bits = global_bits
        self.all_bits = local_bits + global_bits
        self.pivot = local_bits - 1 - global_bits
        self.tiles = 1 << (local_bits - ROW_BITS)
        self.rows = self.tiles * TILE
        self.group = 1 << global_bits
        self.chunk = self.rows // self.group
        self.chunked = self.rows % self.group == 0 and self.chunk % TILE == 0

    def first_map(self):
        return {q: ("local", q) if q < self.local_bits else ("device", q - self.local_bits)
                for q in range(self.all_bits)}

    def second_map(self):
        where = {q: ("local", q) for q in range(self.pivot)}
        where[self.local_bits - 1] = ("local", self.pivot)
        for k in range(self.global_bits):
            where[self.local_bits + k] = ("local", self.pivot + 1 + k)
            where[self.pivot if k == self.global_bits - 1 else self.pivot + 1 + k] = ("device", k)
        return where

    def moved_map(self):
        return {pos: self.pivot if pos == self.local_bits - 1 else pos
                for pos in range(self.pivot + 1, self.local_bits)}


def lane_iota():
    return lax.broadcasted_iota(jnp.int32, (TILE, 128), 1)


def sub_iota():
    return lax.broadcasted_iota(jnp.int32, (TILE, 128), 0)


def bit_of(pos):
    if pos < LANE_BITS:
        return lane_iota() >> pos & 1
    return sub_iota() >> (pos - LANE_BITS) & 1


def sign_of(pos):
    return (1 - 2 * bit_of(pos)).astype(jnp.float32)


def shift_up(x, pos):
    if pos < LANE_BITS:
        return pltpu.roll(x, 128 - (1 << pos), 1)
    return pltpu.roll(x, TILE - (1 << (pos - LANE_BITS)), 0)


def shift_down(x, pos):
    if pos < LANE_BITS:
        return pltpu.roll(x, 1 << pos, 1)
    return pltpu.roll(x, 1 << (pos - LANE_BITS), 0)


def flip(x, pos):
    if pos in (LANE_BITS - 1, ROW_BITS - 1):
        return shift_down(x, pos)
    return jnp.where(bit_of(pos) == 0, shift_up(x, pos), shift_down(x, pos))


def entangle(amp, all_bits):
    x = amp & (amp >> 1 | (amp & 1) << (all_bits - 1))
    step = 16
    while step:
        x = x ^ x >> step
        step //= 2
    return (1 - 2 * (x & 1)).astype(jnp.float32)


def tile_signs(frame, amp_of):
    if frame.pivot >= ROW_BITS:
        return [entangle(amp_of(t), frame.all_bits) for t in range(frame.tiles)]
    edge = 1 | frame.tiles >> 1
    made, signs = {}, []
    for t in range(frame.tiles):
        key = t & edge
        if key not in made:
            sign = entangle(amp_of(key), frame.all_bits)
            made[key] = (sign, -sign)
        signs.append(made[key][odd(t & t >> 1) ^ odd(key & key >> 1)])
    return signs


def position_index(tile):
    return tile << ROW_BITS | sub_iota() << LANE_BITS | lane_iota()


def swap_pivot(tiles, frame):
    half = len(tiles) // 2
    pos = frame.pivot
    out = list(tiles)
    for t in range(half):
        low, high = tiles[t], tiles[t + half]
        if pos >= ROW_BITS:
            bit = 1 << (pos - ROW_BITS)
            if t & bit:
                out[t], out[t - bit + half] = tiles[t - bit + half], tiles[t]
        else:
            keep = bit_of(pos) == 0
            out[t] = jnp.where(keep, low, shift_down(high, pos))
            out[t + half] = jnp.where(keep, shift_up(low, pos), high)
    return out


def polynomial(x, coefficients):
    total = jnp.full_like(x, coefficients[-1])
    for value in coefficients[-2::-1]:
        total = total * x + value
    return total


def half_turn(angle):
    x = jnp.full((TILE, 128), 0.5, jnp.float32) * angle
    square = x * x
    cosine = polynomial(square, [(-1) ** k / math.factorial(2 * k) for k in range(9)])
    sine = x * polynomial(square, [(-1) ** k / math.factorial(2 * k + 1) for k in range(8)])
    return cosine, sine


class Params:
    def __init__(self, angles, kinds, layers):
        self.kinds = kinds
        self.layers = layers
        self.turns = {}
        self.angles = angles

    def turn(self, layer, kind):
        if (layer, kind) not in self.turns:
            self.turns[layer, kind] = half_turn(self.angles[layer, kind])
        return self.turns[layer, kind]

    def gate(self, layer, qubit):
        kind = self.kinds[layer, qubit]
        (c0, s0), (c1, s1), (c2, s2) = [self.turn(layer, k) for k in range(3)]
        is_z = kind == 2
        c = jnp.where(is_z, c2, jnp.where(kind == 1, c1, c0))
        sy = jnp.where(is_z, 0.0, jnp.where(kind == 1, s1, s0))
        return c, sy, jnp.where(is_z, s2, 0.0)

    def pick(self, layer, qubit, kind):
        return jnp.where(self.kinds[layer, qubit] == kind, 0.5, 0.0)


def turn(re, im, gate, pos, low_tile_bit):
    c, sy, sz = gate
    if pos < ROW_BITS:
        z = sign_of(pos)
        y_part, z_part = sy * z, sz * z
        new_re = [c * a + y_part * flip(a, pos) - z_part * b for a, b in zip(re, im)]
        new_im = [c * b + y_part * flip(b, pos) + z_part * a for a, b in zip(re, im)]
        return new_re, new_im
    bit = 1 << (pos - ROW_BITS - low_tile_bit)
    new_re, new_im = list(re), list(im)
    for t in range(len(re)):
        if t & bit:
            continue
        u = t | bit
        new_re[t] = c * re[t] + sy * re[u] - sz * im[t]
        new_im[t] = c * im[t] + sy * im[u] + sz * re[t]
        new_re[u] = c * re[u] - sy * re[t] + sz * im[u]
        new_im[u] = c * im[u] - sy * im[t] - sz * re[u]
    return new_re, new_im


def sweep(loads, stores, frame, gates):
    tile_bits = frame.tiles.bit_length() - 1
    low = min(3, tile_bits)
    span = 1 << low
    near = [pos for pos in sorted(gates) if LANE_BITS <= pos < ROW_BITS + low]
    far = [pos for pos in sorted(gates) if pos >= ROW_BITS + low]
    load, store = loads, stores
    plans = []
    if near:
        plans.append((near, 0, [[base * span + t for t in range(span)]
                                for base in range(frame.tiles // span)]))
    if far:
        plans.append((far, low, [[base + t * span for t in range(frame.tiles // span)]
                                 for base in range(span)]))
    for positions, low_bit, blocks in plans:
        for block in blocks:
            pairs = [load(t) for t in block]
            re, im = [a for a, _ in pairs], [b for _, b in pairs]
            for pos in positions:
                re, im = turn(re, im, gates[pos], pos, low_bit)
            for t, a, b in zip(block, re, im):
                store(t, a, b)


def split(x):
    high = x.astype(jnp.bfloat16)
    return high, (x - high.astype(jnp.float32)).astype(jnp.bfloat16)


def lane_matrix(params, layer, qubits):
    out = lane_iota()
    blocks = None
    for pos, qubit in enumerate(qubits):
        c, sy, sz = params.gate(layer, qubit)
        upper = out >> pos & 1
        z = (1 - 2 * upper).astype(jnp.float32)
        y_part, z_part = sy * z, sz * z

        def entry(same):
            return jnp.where(same, c, y_part), jnp.where(same, z_part, 0.0)

        if pos < 3:
            options = [entry((sub_iota() >> pos & 1) == upper)]
        else:
            options = [entry(upper == 0), entry(upper == 1)]
        if blocks is None:
            blocks = options
        else:
            blocks = [(real * g_real - imag * g_imag, real * g_imag + imag * g_real)
                      for g_real, g_imag in options for real, imag in blocks]
    real = jnp.concatenate([block[0] for block in blocks], axis=0)
    imag = jnp.concatenate([block[1] for block in blocks], axis=0)
    top = jnp.concatenate([real, imag], axis=1)
    bottom = jnp.concatenate([-imag, real], axis=1)
    return jnp.concatenate([top, bottom], axis=0)


def lane_turn(x, matrix):
    x_high, x_low = split(x)
    m_high, m_low = split(matrix)
    dot = functools.partial(jnp.dot, preferred_element_type=jnp.float32)
    return dot(x_high, m_high) + (dot(x_low, m_high) + dot(x_high, m_low))


def parts_of(where, qubit, device):
    kind, pos = where[qubit]
    if kind == "device":
        return None, None, (1 - 2 * (device >> pos & 1)).astype(jnp.float32)
    if pos >= ROW_BITS:
        return 1 << (pos - ROW_BITS), None, None
    return None, sign_of(pos), None


def odd(x):
    return bin(x).count("1") & 1


def gather_terms(frame, where, qubits, load_ket, load_bra, params, device):
    n = frame.all_bits
    layers = params.layers
    zero = jnp.zeros((TILE, 128), jnp.float32)
    near, far = [], []
    for q in qubits:
        (far if where[q][1] >= ROW_BITS else near).append(q)
    ratio_mask = {}
    for q in qubits:
        mask = 0
        for other in ((q - 1) % n, (q + 1) % n):
            kind, pos = where[other]
            if kind == "local" and pos >= ROW_BITS:
                mask ^= 1 << (pos - ROW_BITS)
        ratio_mask[q] = mask
    buckets = {q: [None, None] for q in qubits}

    def add(q, side, value):
        old = buckets[q][side]
        buckets[q][side] = value if old is None else old + value

    phases = []
    for t in range(frame.tiles):
        ket_re, ket_im = load_ket(t)
        bra_re, bra_im = load_bra(t)
        phases.append(bra_re * ket_im - bra_im * ket_re)
        for q in near:
            pos = where[q][1]
            value = bra_re * flip(ket_re, pos) + bra_im * flip(ket_im, pos)
            add(q, odd(t & ratio_mask[q]), value)
    for q in far:
        bit = 1 << (where[q][1] - ROW_BITS)
        for t in range(frame.tiles):
            if t & bit:
                continue
            ket_low, ket_high = load_ket(t), load_ket(t | bit)
            bra_low, bra_high = load_bra(t), load_bra(t | bit)
            value = (bra_high[0] * ket_low[0] + bra_high[1] * ket_low[1]) - (
                bra_low[0] * ket_high[0] + bra_low[1] * ket_high[1])
            add(q, odd(t & ratio_mask[q]), value)
    signed = {}
    level = phases
    bit = frame.tiles // 2
    while bit:
        diffs = [level[t] - level[t + bit] for t in range(bit)]
        while len(diffs) > 1:
            half = len(diffs) // 2
            diffs = [diffs[t] + diffs[t + half] for t in range(half)]
        signed[bit] = diffs[0]
        level = [level[t] + level[t + bit] for t in range(bit)]
        bit //= 2
    total = level[0]
    sums = [[zero, zero, zero] for _ in range(layers)]
    for q in qubits:
        pos = where[q][1]
        plus, minus = [zero if b is None else b for b in buckets[q]]
        if pos < ROW_BITS:
            z = sign_of(pos)
            phase = total * z
            last = (plus + minus) * -z
            first = (plus - minus) * -z
        else:
            phase = signed[1 << (pos - ROW_BITS)]
            last = plus + minus
            first = plus - minus
        for other in ((q - 1) % n, (q + 1) % n):
            _, vector, scalar = parts_of(where, other, device)
            if vector is not None:
                first = first * vector
            if scalar is not None:
                first = first * scalar
        for layer in range(layers):
            y_term = last if layer == layers - 1 else first
            for kind in range(2):
                sums[layer][kind] = sums[layer][kind] + params.pick(layer, q, kind) * y_term
            sums[layer][2] = sums[layer][2] + params.pick(layer, q, 2) * phase
    return sums


def one_row(tile):
    for step in (64, 32, 16):
        tile = tile + pltpu.roll(tile, step, 1)
    return jnp.sum(jnp.where(lane_iota() >> 4 == sub_iota(), tile, 0.0), axis=0, keepdims=True)


def rows_of(sums):
    flat = [jnp.sum(tile, axis=0, keepdims=True) for layer in sums for tile in layer]
    flat += [jnp.zeros((1, 128), jnp.float32)] * (TILE - len(flat))
    return jnp.concatenate(flat, axis=0)


def back_ref(frame, comp):
    def at(t):
        if frame.chunked:
            per = frame.chunk // TILE
            start = t // per * (2 * frame.chunk + 1) + comp * frame.chunk + t % per * TILE
            return (pl.ds(start, TILE), slice(None))
        return (comp, pl.ds(t * TILE, TILE), slice(None))
    return at


def tile_ref(frame, comp):
    def at(t):
        if frame.chunked:
            per = frame.chunk // TILE
            start = comp * frame.chunk + t % per * TILE
            return (t // per, pl.ds(start, TILE), slice(None))
        return (comp, pl.ds(t * TILE, TILE), slice(None))
    return at


def scratch_io(ref, frame, state):
    base = state * frame.rows

    def load(t):
        rows = pl.ds(base + t * TILE, TILE)
        return ref[rows, 0:128], ref[rows, 128:256]

    def store(t, re, im):
        rows = pl.ds(base + t * TILE, TILE)
        ref[rows, 0:128] = re
        ref[rows, 128:256] = im

    return load, store


def first_kernel(frame, layers, dev_ref, angles, kinds, ket_ref, obs_ref, out_ref, sums_ref, *scratch):
    work, staged, done = scratch
    device = dev_ref[0]
    params = Params(angles, kinds, layers)
    layer = layers - 1
    scale = 2.0 / math.sqrt(1 << frame.all_bits)
    load_ket, store_ket = scratch_io(work, frame, 0)
    load_bra, store_bra = scratch_io(work, frame, 1)
    signs = tile_signs(
        frame, lambda t: device << frame.local_bits | position_index(t))
    matrix = lane_matrix(params, layer, range(LANE_BITS))
    gates = {pos: params.gate(layer, pos) for pos in range(LANE_BITS, frame.local_bits)}
    copies = []

    def finish(state, load, store):
        rows = pl.ds(state * frame.rows, frame.rows)
        work[rows, :] = lane_turn(work[rows, :], matrix)
        sweep(load, store, frame, gates)
        pairs = [load(t) for t in range(frame.tiles)]
        for part in range(2):
            tiles = swap_pivot([pair[part] for pair in pairs], frame)
            at = tile_ref(frame, 2 * state + part)
            for t in range(frame.tiles):
                staged[at(t)] = tiles[t]
        if frame.chunked:
            span = (slice(None), pl.ds(2 * state * frame.chunk, 2 * frame.chunk))
        else:
            span = (pl.ds(2 * state, 2),)
        copy = pltpu.make_async_copy(staged.at[span], out_ref.at[span], done.at[state])
        copy.start()
        copies.append(copy)

    for t in range(frame.tiles):
        re = ket_ref[pl.ds(2 * TILE * t, TILE, stride=2), :] * signs[t]
        im = ket_ref[pl.ds(2 * TILE * t + 1, TILE, stride=2), :] * signs[t]
        store_ket(t, re, im)
        factor = obs_ref[pl.ds(TILE * t, TILE), :] * scale
        store_bra(t, re * factor, im * factor)
    finish(0, load_ket, store_ket)
    finish(1, load_bra, store_bra)
    moved = list(range(frame.pivot, frame.local_bits - 1))
    sums = gather_terms(frame, frame.first_map(), moved, load_ket, load_bra, params, device)
    sums_ref[...] = rows_of(sums)
    for copy in copies:
        copy.wait()


def middle_kernel(frame, layers, dev_ref, angles, kinds, in_ref, sums_ref, out_ref, work, *flat_out):
    device = dev_ref[0]
    params = Params(angles, kinds, layers)
    load_ket, store_ket = scratch_io(work, frame, 0)
    load_bra, store_bra = scratch_io(work, frame, 1)
    where = frame.second_map()
    placed = {pos: q for q, (kind, pos) in where.items() if kind == "local"}
    at = [tile_ref(frame, comp) for comp in range(4)]
    for t in range(frame.tiles):
        store_ket(t, in_ref[at[0](t)], in_ref[at[1](t)])
        store_bra(t, in_ref[at[2](t)], in_ref[at[3](t)])
    assert frame.pivot + 1 >= LANE_BITS
    gates = {pos: params.gate(layers - 1, placed[pos])
             for pos in range(frame.pivot + 1, frame.local_bits)}
    sweep(load_ket, store_ket, frame, gates)
    sweep(load_bra, store_bra, frame, gates)
    qubits = [placed[pos] for pos in range(frame.local_bits)]
    sums = gather_terms(frame, where, qubits, load_ket, load_bra, params, device)
    partial = one_row(sums_ref[...] + rows_of(sums))
    g = frame.global_bits
    high = device >> (g - 1) & 1
    base = (device & (1 << (g - 1)) - 1) << (frame.pivot + 1) | high << frame.pivot

    def amp_of(t):
        pos = position_index(t)
        return (base | pos & (1 << frame.pivot) - 1
                | (pos >> frame.pivot & 1) << (frame.local_bits - 1)
                | pos >> (frame.pivot + 1) << frame.local_bits)

    signs = tile_signs(frame, amp_of)
    for t in range(frame.tiles):
        re, im = load_bra(t)
        store_bra(t, re * signs[t], im * signs[t])
    bra_rows = pl.ds(frame.rows, frame.rows)
    lane_on = [placed[pos] for pos in range(LANE_BITS)]
    work[bra_rows, :] = lane_turn(work[bra_rows, :], lane_matrix(params, 0, lane_on))
    gates = {pos: params.gate(0, placed[pos]) for pos in range(LANE_BITS, frame.local_bits)}
    sweep(load_bra, store_bra, frame, gates)
    at = [back_ref(frame, comp) for comp in range(2)]
    for t in range(frame.tiles):
        re, im = load_bra(t)
        out_ref[at[0](t)] = re
        out_ref[at[1](t)] = im
    if frame.chunked:
        for j in range(frame.group):
            row = (j + 1) * (2 * frame.chunk + 1) - 1
            out_ref[pl.ds(row, 1), :] = partial
    else:
        flat_out[0][...] = partial


def last_kernel(frame, layers, angles, kinds, in_ref, *refs):
    *sums_ref, bra_ref, grads_ref, work = refs
    params = Params(angles, kinds, layers)
    load, store = scratch_io(work, frame, 0)
    at = [back_ref(frame, comp) for comp in range(2)]
    for t in range(frame.tiles):
        store(t, in_ref[at[0](t)], in_ref[at[1](t)])
    gates = {pos: params.gate(0, q) for pos, q in frame.moved_map().items()}
    sweep(load, store, frame, gates)
    pairs = [load(t) for t in range(frame.tiles)]
    for part in range(2):
        tiles = swap_pivot([pair[part] for pair in pairs], frame)
        for t in range(frame.tiles):
            bra_ref[pl.ds(2 * TILE * t + part, TILE, stride=2), :] = tiles[t]
    if frame.chunked:
        step = 2 * frame.chunk + 1
        rows = in_ref[pl.ds(step - 1, frame.group, stride=step), :]
    else:
        rows = sums_ref[0][:, 0, :]
    total = jnp.sum(rows, axis=0, keepdims=True)
    owner = lax.broadcasted_iota(jnp.int32, (1, 128), 1) >> 4
    for layer in range(layers):
        for kind in range(3):
            own = jnp.where(owner == 3 * layer + kind, total, 0.0)
            grads_ref[layer, kind] = jnp.sum(own)


def on_device(ket_state, observable, angles, gate_kinds):
    amp_count = ket_state.shape[1]
    local_bits = amp_count.bit_length() - 1
    group = lax.axis_size("amp")
    frame = Frame(local_bits, group.bit_length() - 1)
    layers = angles.shape[0]
    rows = frame.rows
    device = lax.axis_index("amp").astype(jnp.int32).reshape(1)
    smem = pl.BlockSpec(memory_space=pltpu.SMEM)
    vmem = pl.BlockSpec(memory_space=pltpu.VMEM)
    f32 = jnp.float32

    def flat(comps):
        return jax.ShapeDtypeStruct((comps, rows, 128), f32)

    def exchange(x):
        return lax.all_to_all(x, "amp", 0, 0, tiled=True)

    def to_chunks(x):
        comps = x.shape[0]
        return x.reshape(comps, group, rows * 128 // group).transpose(1, 0, 2)

    def from_chunks(x):
        return x.transpose(1, 0, 2).reshape(x.shape[1], rows, 128)

    ket_rows = ket_state.reshape(2, rows, 128).transpose(1, 0, 2).reshape(2 * rows, 128)
    obs_rows = observable.reshape(rows, 128)
    work = pltpu.VMEM((2 * rows, 256), f32)
    tile = jax.ShapeDtypeStruct((TILE, 128), f32)
    sent_shape = flat(4)
    if frame.chunked:
        sent_shape = jax.ShapeDtypeStruct((group, 4 * frame.chunk, 128), f32)
    sent, sums = pl.pallas_call(
        functools.partial(first_kernel, frame, layers),
        in_specs=[smem, smem, smem, vmem, vmem],
        out_specs=(pl.BlockSpec(memory_space=pl.ANY), vmem),
        out_shape=(sent_shape, tile),
        scratch_shapes=[work, pltpu.VMEM(sent_shape.shape, f32), pltpu.SemaphoreType.DMA((2,))],
        name="first_kernel",
    )(device, angles, gate_kinds, ket_rows, obs_rows)
    if frame.chunked:
        got = exchange(sent)
    else:
        got = from_chunks(exchange(to_chunks(sent)))
    step = 2 * frame.chunk + 1
    if frame.chunked:
        outs = (jax.ShapeDtypeStruct((group * step, 128), f32),)
    else:
        outs = (flat(2), jax.ShapeDtypeStruct((1, 128), f32))
    back = pl.pallas_call(
        functools.partial(
            middle_kernel if frame.chunked else middle_flat, frame, layers),
        in_specs=[smem, smem, smem, vmem, vmem],
        out_specs=(vmem,) * len(outs),
        out_shape=outs,
        scratch_shapes=[work],
        name="middle_kernel",
    )(device, angles, gate_kinds, got, sums)
    if frame.chunked:
        final = exchange(back[0].reshape(group, step, 1, 128)).reshape(group * step, 128)
        operands = (final,)
    else:
        final = from_chunks(exchange(to_chunks(back[0])))
        operands = (final, lax.all_gather(back[1], "amp"))
    bra_rows, grads = pl.pallas_call(
        functools.partial(last_kernel, frame, layers),
        in_specs=[smem, smem] + [vmem] * len(operands),
        out_specs=(vmem, smem),
        out_shape=(jax.ShapeDtypeStruct((2 * rows, 128), f32),
                   jax.ShapeDtypeStruct((layers, 3), f32)),
        scratch_shapes=[pltpu.VMEM((rows, 256), f32)],
        name="last_kernel",
    )(angles, gate_kinds, *operands)
    bra = bra_rows.reshape(rows, 2, 128).transpose(1, 0, 2).reshape(2, amp_count)
    return bra, grads


def middle_flat(frame, layers, dev_ref, angles, kinds, in_ref, sums_ref, out_ref, part_ref, work):
    middle_kernel(frame, layers, dev_ref, angles, kinds, in_ref, sums_ref, out_ref, work, part_ref)


def solution(mesh):
    placed = (P(None, "amp"), P("amp"), P(), P())
    return jax.shard_map(
        on_device, mesh=mesh, in_specs=placed, out_specs=(P(None, "amp"), P()), check_vma=False
    )
```
